256 devices in a mesh: lon: 16 (over x_lo, z), lat: 16 (over x_hi, y, core).
Axes of the slice: x: 4 (x_hi: 2, x_lo: 2; x = x_hi * 2 + x_lo), y: 4, z: 8, core: 2. Of those that a mesh axis runs over, the one named last changes fastest.
Arguments:
- grid_field: float32 [4, 256, 16, 2048], P(None, 'lat', None, 'lon'), may hold values from -6 to 6
- lat_weight: float32 [256], replicated, may hold values from 0.3 to 3
Outputs:
- spec_real: float32 [4, 256, 16, 1024], P(None, None, 'lat', 'lon')
- spec_imag: float32 [4, 256, 16, 1024], P(None, None, 'lat', 'lon')
The draws below stay inside these ranges and needn't reach their ends.
All inputs are finite; a program needn't handle non-finite values.
Results may differ from the reference program's by a relative error of at most 0.000071.
Values sent between devices are 32-bit elements; how exact they have to be, the bound alone decides.
No kernel may reach another device: no remote copies, remote signals or barrier semaphores. Data moves between devices by JAX's collectives and lax.ppermute only.
A program may use at most 64 MiB of HBM per device.

```python
import math
import jax
import jax.numpy as jnp

NLON = 2048
MODES = 1024
F = 4
R = 16
NLAT = 256


def shard_levels(key, dims, shards, smallest, high):
    def one(position, parts):
        steps = jax.random.uniform(jax.random.fold_in(jax.random.fold_in(key, 6), position), (parts,), jnp.float32, smallest / len(shards), high / len(shards))
        return jnp.repeat(jnp.exp(steps), dims[position] // parts).reshape((-1,) + (1,) * (len(dims) - position - 1))

    factor_of = one(*shards[0])
    for cut in shards[1:]:
        factor_of = factor_of * one(*cut)
    return factor_of


def scatter_about(stream_key, shape, scale, limit, cuts=(), dtype=jnp.bfloat16):
    array = scale * jax.random.normal(stream_key, shape, jnp.float32)
    if cuts:
        array = array * shard_levels(stream_key, shape, cuts, -0.22, 0.18)
    return jnp.clip(array, -limit, limit).astype(dtype)


def setup_inputs(seed: int = 0) -> dict:
    seeds = jax.random.split(jax.random.key(seed), 3)
    grid_field = scatter_about(seeds[0], (F, NLAT, R, NLON), 1.0, 6.0, ((1, 16), (3, 16)), jnp.float32)
    lat_weight = jnp.clip(jnp.exp(jax.random.uniform(seeds[1], (NLAT,), jnp.float32, math.log(0.3), math.log(3.0))), 0.3, 3.0)
    return dict(grid_field=grid_field, lat_weight=lat_weight)


def reference(grid_field, lat_weight):
    normalizer = 1.0 / math.sqrt(NLON)
    spectra = jnp.fft.rfft(grid_field, axis=-1)[..., :MODES] * normalizer
    weights_row = lat_weight[None, :, None, None]
    spec_real = (jnp.real(spectra) * weights_row).astype(jnp.float32)
    spec_imag = (jnp.imag(spectra) * weights_row).astype(jnp.float32)
    return (spec_real, spec_imag)
```

```python
import functools
import math

import jax
import jax.numpy as jnp
import numpy as np
from jax import lax
from jax.experimental import pallas as pl
from jax.experimental.pallas import tpu as pltpu
from jax.sharding import PartitionSpec as P

LENGTH = 2048
PEERS = 16
BLOCK = 128
ROWS = 64


def mode_tables():
    b = np.arange(BLOCK)
    tables = np.zeros((8, 256, 256))
    for residue in range(PEERS):
        group, e = np.divmod(np.arange(128), 8)
        part, step = np.divmod(e, 4)
        owner = (group - residue) % PEERS
        mode = residue + PEERS * (4 * owner + step)
        phase = 2.0 * math.pi * (b[:, None] * mode[None, :] % LENGTH) / LENGTH
        cosine = np.cos(phase) / math.sqrt(LENGTH)
        sine = np.sin(phase) / math.sqrt(LENGTH)
        sign = -1.0 if residue > 8 else 1.0
        from_real = np.where(part == 0, cosine, -sine)
        from_imag = sign * np.where(part == 0, sine, cosine)
        if residue == 0:
            tables[0, :128, :128] = from_real
        elif residue == 8:
            tables[0, 128:, 128:] = from_real
        else:
            tile = min(residue, PEERS - residue)
            at = 0 if residue < 8 else 128
            tables[tile, :128, at : at + 128] = from_real
            tables[tile, 128:, at : at + 128] = from_imag
    table = tables.astype(np.float32)
    high = table.astype(jnp.bfloat16)
    low = (table - high.astype(np.float32)).astype(jnp.bfloat16)
    return np.stack([high, low])


def real_dft16(x):
    h = math.sqrt(0.5)
    c1, c3 = math.cos(math.pi / 8), math.cos(3 * math.pi / 8)
    s1, s3 = math.sin(math.pi / 8), math.sin(3 * math.pi / 8)
    s = [x[a] + x[a + 8] for a in range(8)]
    d = [x[a] - x[a + 8] for a in range(8)]
    p = [s[a] + s[a + 4] for a in range(4)]
    q = [s[a] - s[a + 4] for a in range(4)]
    out = [None] * 9
    even, odd = p[0] + p[2], p[1] + p[3]
    out[0] = (even + odd, None)
    out[8] = (even - odd, None)
    out[4] = (p[0] - p[2], p[3] - p[1])
    diff, total = h * (q[1] - q[3]), h * (q[1] + q[3])
    out[2] = (q[0] + diff, -q[2] - total)
    out[6] = (q[0] - diff, q[2] - total)
    e1, e2, e3 = d[1] - d[7], h * (d[2] - d[6]), d[3] - d[5]
    g1, g2, g3 = d[1] + d[7], h * (d[2] + d[6]), d[3] + d[5]
    r1, r3 = d[0] + e2, d[0] - e2
    u1, u3 = c1 * e1 + c3 * e3, c3 * e1 - c1 * e3
    i1, i3 = g2 + d[4], g2 - d[4]
    v1, v3 = s1 * g1 + s3 * g3, s3 * g1 - s1 * g3
    out[1] = (r1 + u1, -(v1 + i1))
    out[7] = (r1 - u1, i1 - v1)
    out[3] = (r3 + u3, -(v3 + i3))
    out[5] = (r3 - u3, i3 - v3)
    return out


def transform_kernel(y_ref, table_ref, o_ref, lhs, mid):
    for g in range(ROWS // 16):
        rows = slice(16 * g, 16 * g + 16)
        dft = real_dft16([y_ref[a, rows, :] for a in range(PEERS)])
        for tile in range(8):
            pair = (dft[0][0], dft[8][0]) if tile == 0 else dft[tile]
            for part in range(2):
                high = pair[part].astype(jnp.bfloat16)
                low = (pair[part] - high.astype(jnp.float32)).astype(jnp.bfloat16)
                at = slice(128 * part, 128 * part + 128)
                lhs[tile, 16 * g : 16 * g + 16, at] = high
                lhs[tile, ROWS + 16 * g : ROWS + 16 * g + 16, at] = low
    dot = functools.partial(jnp.dot, preferred_element_type=jnp.float32)
    for tile in range(8):
        both = dot(lhs[tile], table_ref[0, tile])
        total = both[:ROWS] + both[ROWS:] + dot(lhs[tile, :ROWS, :], table_ref[1, tile])
        mid[tile] = total[:, :128]
        mid[8 if tile == 0 else PEERS - tile] = total[:, 128:]
    group = lax.broadcasted_iota(jnp.int32, (8, 128), 1) // 8
    bits = [(group >> s) % 2 == 1 for s in range(4)]
    for g in range(ROWS // 8):
        v = [mid[k, 8 * g : 8 * g + 8, :] for k in range(PEERS)]
        for s in range(4):
            v = [jnp.where(bits[s], v[(i + (1 << s)) % PEERS], v[i]) for i in range(PEERS)]
        latitude, radius = g // 2, 8 * (g % 2)
        for j in range(PEERS):
            value = v[-j % PEERS]
            if j:
                value = pltpu.roll(value, 128 - 8 * j, 1)
            o_ref[pl.ds(radius * 64 + j * 4 + latitude, 8, stride=64), :] = value


def transform(y):
    return pl.pallas_call(
        transform_kernel,
        out_shape=jax.ShapeDtypeStruct((1024, 128), jnp.float32),
        in_specs=[pl.BlockSpec(memory_space=pltpu.VMEM)] * 2,
        out_specs=pl.BlockSpec(memory_space=pltpu.VMEM),
        scratch_shapes=[
            pltpu.VMEM((8, 2 * ROWS, 256), jnp.bfloat16),
            pltpu.VMEM((PEERS, ROWS, 128), jnp.float32),
        ],
        compiler_params=pltpu.CompilerParams(vmem_limit_bytes=16 << 20),
        cost_estimate=pl.CostEstimate(flops=2 * 8 * 192 * 256 * 256, bytes_accessed=3 << 20, transcendentals=0),
        name="transform",
    )(y, jnp.asarray(mode_tables()))


def weigh_kernel(g_ref, w_ref, re_ref, im_ref, turned):
    weights = w_ref[...]
    for f in range(4):
        rows = jnp.concatenate([g_ref[64 * i + 16 * f : 64 * i + 16 * f + 16, :] for i in range(16)], axis=0)
        for half in range(2):
            turned[half] = rows[128 * half : 128 * half + 128].T * weights[:, 128 * half : 128 * half + 128]
        for half in range(2):
            at = slice(128 * half, 128 * half + 128)
            for step in range(4):
                re_ref[f, 16 * step : 16 * step + 16, at] = turned[half, pl.ds(step, 16, stride=8), :]
                im_ref[f, 16 * step : 16 * step + 16, at] = turned[half, pl.ds(4 + step, 16, stride=8), :]


def weigh(g, lat_weight):
    shape = jax.ShapeDtypeStruct((4, 64, 256), jnp.float32)
    return pl.pallas_call(
        weigh_kernel,
        out_shape=(shape, shape),
        in_specs=[pl.BlockSpec(memory_space=pltpu.VMEM)] * 2,
        out_specs=(pl.BlockSpec(memory_space=pltpu.VMEM),) * 2,
        scratch_shapes=[pltpu.VMEM((2, 128, 128), jnp.float32)],
        compiler_params=pltpu.CompilerParams(vmem_limit_bytes=16 << 20),
        cost_estimate=pl.CostEstimate(flops=1 << 18, bytes_accessed=1 << 20, transcendentals=0),
        name="weigh",
    )(g, lat_weight.reshape(1, 256))


def per_device(grid_field, lat_weight):
    y = lax.all_to_all(grid_field.reshape(16, 64, 128), "lon", 0, 0, tiled=True)
    z = transform(y)
    g = lax.all_to_all(z.reshape(256, 4, 128), ("lat", "lon"), 0, 0, tiled=True)
    real, imag = weigh(g.reshape(1024, 128), lat_weight)
    return tuple(part.transpose(0, 2, 1)[:, :, None, :] for part in (real, imag))


def solution(mesh):
    in_specs = (P(None, "lat", None, "lon"), P())
    out_specs = (P(None, None, "lat", "lon"), P(None, None, "lat", "lon"))
    return jax.shard_map(per_device, mesh=mesh, in_specs=in_specs, out_specs=out_specs, check_vma=False)
```

```python
import functools
import math

import jax
import jax.numpy as jnp
import numpy as np
from jax import lax
from jax.experimental import pallas as pl
from jax.experimental.pallas import tpu as pltpu
from jax.sharding import PartitionSpec as P

LENGTH = 2048
PEERS = 16
BLOCK = 128
ROWS = 64


def mode_tables():
    b = np.arange(BLOCK)
    tables = np.zeros((8, 256, 256))
    for residue in range(PEERS):
        group, e = np.divmod(np.arange(128), 8)
        part, step = np.divmod(e, 4)
        owner = (group - residue) % PEERS
        mode = residue + PEERS * (4 * owner + step)
        phase = 2.0 * math.pi * (b[:, None] * mode[None, :] % LENGTH) / LENGTH
        cosine = np.cos(phase) / math.sqrt(LENGTH)
        sine = np.sin(phase) / math.sqrt(LENGTH)
        sign = -1.0 if residue > 8 else 1.0
        from_real = np.where(part == 0, cosine, -sine)
        from_imag = sign * np.where(part == 0, sine, cosine)
        if residue == 0:
            tables[0, :128, :128] = from_real
        elif residue == 8:
            tables[0, 128:, 128:] = from_real
        else:
            tile = min(residue, PEERS - residue)
            at = 0 if residue < 8 else 128
            tables[tile, :128, at : at + 128] = from_real
            tables[tile, 128:, at : at + 128] = from_imag
    table = tables.astype(np.float32)
    high = table.astype(jnp.bfloat16)
    low = (table - high.astype(np.float32)).astype(jnp.bfloat16)
    return np.stack([high, low])


def real_dft16(x):
    h = math.sqrt(0.5)
    c1, c3 = math.cos(math.pi / 8), math.cos(3 * math.pi / 8)
    s1, s3 = math.sin(math.pi / 8), math.sin(3 * math.pi / 8)
    s = [x[a] + x[a + 8] for a in range(8)]
    d = [x[a] - x[a + 8] for a in range(8)]
    p = [s[a] + s[a + 4] for a in range(4)]
    q = [s[a] - s[a + 4] for a in range(4)]
    out = [None] * 9
    even, odd = p[0] + p[2], p[1] + p[3]
    out[0] = (even + odd, None)
    out[8] = (even - odd, None)
    out[4] = (p[0] - p[2], p[3] - p[1])
    diff, total = h * (q[1] - q[3]), h * (q[1] + q[3])
    out[2] = (q[0] + diff, -q[2] - total)
    out[6] = (q[0] - diff, q[2] - total)
    e1, e2, e3 = d[1] - d[7], h * (d[2] - d[6]), d[3] - d[5]
    g1, g2, g3 = d[1] + d[7], h * (d[2] + d[6]), d[3] + d[5]
    r1, r3 = d[0] + e2, d[0] - e2
    u1, u3 = c1 * e1 + c3 * e3, c3 * e1 - c1 * e3
    i1, i3 = g2 + d[4], g2 - d[4]
    v1, v3 = s1 * g1 + s3 * g3, s3 * g1 - s1 * g3
    out[1] = (r1 + u1, -(v1 + i1))
    out[7] = (r1 - u1, i1 - v1)
    out[3] = (r3 + u3, -(v3 + i3))
    out[5] = (r3 - u3, i3 - v3)
    return out


def transform_kernel(y_ref, table_ref, o_ref, lhs, mid):
    for g in range(ROWS // 16):
        rows = slice(16 * g, 16 * g + 16)
        dft = real_dft16([y_ref[a, rows, :] for a in range(PEERS)])
        for tile in range(8):
            pair = (dft[0][0], dft[8][0]) if tile == 0 else dft[tile]
            for part in range(2):
                high = pair[part].astype(jnp.bfloat16)
                low = (pair[part] - high.astype(jnp.float32)).astype(jnp.bfloat16)
                at = slice(128 * part, 128 * part + 128)
                lhs[tile, 16 * g : 16 * g + 16, at] = high
                lhs[tile, ROWS + 16 * g : ROWS + 16 * g + 16, at] = low
    dot = functools.partial(jnp.dot, preferred_element_type=jnp.float32)
    for tile in range(8):
        both = dot(lhs[tile], table_ref[0, tile])
        total = both[:ROWS] + both[ROWS:] + dot(lhs[tile, :ROWS, :], table_ref[1, tile])
        mid[tile] = total[:, :128]
        mid[8 if tile == 0 else PEERS - tile] = total[:, 128:]
    group = lax.broadcasted_iota(jnp.int32, (8, 128), 1) // 8
    bits = [(group >> s) % 2 == 1 for s in range(4)]
    for g in range(ROWS // 8):
        v = [mid[k, 8 * g : 8 * g + 8, :] for k in range(PEERS)]
        for s in range(4):
            v = [jnp.where(bits[s], v[(i + (1 << s)) % PEERS], v[i]) for i in range(PEERS)]
        latitude, radius = g // 2, 8 * (g % 2)
        for j in range(PEERS):
            value = v[-j % PEERS]
            if j:
                value = pltpu.roll(value, 128 - 8 * j, 1)
            o_ref[pl.ds(radius * 64 + j * 4 + latitude, 8, stride=64), :] = value


def stage_kernel(table_ref, o_ref, sem):
    copy = pltpu.make_async_copy(table_ref, o_ref, sem)
    copy.start()
    copy.wait()


def stage(table):
    return pl.pallas_call(
        stage_kernel,
        out_shape=jax.ShapeDtypeStruct(table.shape, table.dtype),
        in_specs=[pl.BlockSpec(memory_space=pl.ANY)],
        out_specs=pl.BlockSpec(memory_space=pltpu.VMEM),
        scratch_shapes=[pltpu.SemaphoreType.DMA],
        compiler_params=pltpu.CompilerParams(vmem_limit_bytes=4 << 20),
        cost_estimate=pl.CostEstimate(flops=1 << 24, bytes_accessed=4 << 20, transcendentals=0),
        name="stage",
    )(table)


def transform(y, table):
    return pl.pallas_call(
        transform_kernel,
        out_shape=jax.ShapeDtypeStruct((1024, 128), jnp.float32),
        in_specs=[pl.BlockSpec(memory_space=pltpu.VMEM)] * 2,
        out_specs=pl.BlockSpec(memory_space=pltpu.VMEM),
        scratch_shapes=[
            pltpu.VMEM((8, 2 * ROWS, 256), jnp.bfloat16),
            pltpu.VMEM((PEERS, ROWS, 128), jnp.float32),
        ],
        compiler_params=pltpu.CompilerParams(vmem_limit_bytes=16 << 20),
        cost_estimate=pl.CostEstimate(flops=2 * 8 * 192 * 256 * 256, bytes_accessed=3 << 20, transcendentals=0),
        name="transform",
    )(y, table)


def weigh_kernel(g_ref, w_ref, re_ref, im_ref, turned):
    weights = w_ref[...]
    for f in range(4):
        rows = jnp.concatenate([g_ref[64 * i + 16 * f : 64 * i + 16 * f + 16, :] for i in range(16)], axis=0)
        for half in range(2):
            turned[half] = rows[128 * half : 128 * half + 128].T * weights[:, 128 * half : 128 * half + 128]
        for half in range(2):
            at = slice(128 * half, 128 * half + 128)
            for step in range(4):
                re_ref[f, 16 * step : 16 * step + 16, at] = turned[half, pl.ds(step, 16, stride=8), :]
                im_ref[f, 16 * step : 16 * step + 16, at] = turned[half, pl.ds(4 + step, 16, stride=8), :]


def weigh(g, lat_weight):
    shape = jax.ShapeDtypeStruct((4, 64, 256), jnp.float32)
    return pl.pallas_call(
        weigh_kernel,
        out_shape=(shape, shape),
        in_specs=[pl.BlockSpec(memory_space=pltpu.VMEM)] * 2,
        out_specs=(pl.BlockSpec(memory_space=pltpu.VMEM),) * 2,
        scratch_shapes=[pltpu.VMEM((2, 128, 128), jnp.float32)],
        compiler_params=pltpu.CompilerParams(vmem_limit_bytes=16 << 20),
        cost_estimate=pl.CostEstimate(flops=1 << 18, bytes_accessed=1 << 20, transcendentals=0),
        name="weigh",
    )(g, lat_weight.reshape(1, 256))


def per_device(grid_field, lat_weight):
    y = lax.all_to_all(grid_field.reshape(16, 64, 128), "lon", 0, 0, tiled=True)
    z = transform(y, stage(jnp.asarray(mode_tables())))
    g = lax.all_to_all(z.reshape(256, 4, 128), ("lat", "lon"), 0, 0, tiled=True)
    real, imag = weigh(g.reshape(1024, 128), lat_weight)
    return tuple(part.transpose(0, 2, 1)[:, :, None, :] for part in (real, imag))


def solution(mesh):
    in_specs = (P(None, "lat", None, "lon"), P())
    out_specs = (P(None, None, "lat", "lon"), P(None, None, "lat", "lon"))
    return jax.shard_map(per_device, mesh=mesh, in_specs=in_specs, out_specs=out_specs, check_vma=False)
```

```python
import functools
import math

import jax
import jax.numpy as jnp
import numpy as np
from jax import lax
from jax.experimental import pallas as pl
from jax.experimental.pallas import tpu as pltpu
from jax.sharding import PartitionSpec as P

LENGTH = 2048
PEERS = 16
BLOCK = 128
Z, FAR, NEAR, REST = 128, 64, 32, 4
ROWS = 64


def mode_tables():
    b = np.arange(BLOCK)
    tables = np.zeros((8, 256, 256))
    for residue in range(PEERS):
        group, e = np.divmod(np.arange(128), 8)
        part, step = np.divmod(e, 4)
        owner = (group - residue) % PEERS
        mode = residue + PEERS * (4 * owner + step)
        phase = 2.0 * math.pi * (b[:, None] * mode[None, :] % LENGTH) / LENGTH
        cosine = np.cos(phase) / math.sqrt(LENGTH)
        sine = np.sin(phase) / math.sqrt(LENGTH)
        sign = -1.0 if residue > 8 else 1.0
        from_real = np.where(part == 0, cosine, -sine)
        from_imag = sign * np.where(part == 0, sine, cosine)
        if residue == 0:
            tables[0, :128, :128] = from_real
        elif residue == 8:
            tables[0, 128:, 128:] = from_real
        else:
            tile = min(residue, PEERS - residue)
            at = 0 if residue < 8 else 128
            tables[tile, :128, at : at + 128] = from_real
            tables[tile, 128:, at : at + 128] = from_imag
    table = tables.astype(np.float32)
    high = table.astype(jnp.bfloat16)
    low = (table - high.astype(np.float32)).astype(jnp.bfloat16)
    return np.stack([high, low])


def real_dft16(x):
    h = math.sqrt(0.5)
    c1, c3 = math.cos(math.pi / 8), math.cos(3 * math.pi / 8)
    s1, s3 = math.sin(math.pi / 8), math.sin(3 * math.pi / 8)
    s = [x[a] + x[a + 8] for a in range(8)]
    d = [x[a] - x[a + 8] for a in range(8)]
    p = [s[a] + s[a + 4] for a in range(4)]
    q = [s[a] - s[a + 4] for a in range(4)]
    out = [None] * 9
    even, odd = p[0] + p[2], p[1] + p[3]
    out[0] = (even + odd, None)
    out[8] = (even - odd, None)
    out[4] = (p[0] - p[2], p[3] - p[1])
    diff, total = h * (q[1] - q[3]), h * (q[1] + q[3])
    out[2] = (q[0] + diff, -q[2] - total)
    out[6] = (q[0] - diff, q[2] - total)
    e1, e2, e3 = d[1] - d[7], h * (d[2] - d[6]), d[3] - d[5]
    g1, g2, g3 = d[1] + d[7], h * (d[2] + d[6]), d[3] + d[5]
    r1, r3 = d[0] + e2, d[0] - e2
    u1, u3 = c1 * e1 + c3 * e3, c3 * e1 - c1 * e3
    i1, i3 = g2 + d[4], g2 - d[4]
    v1, v3 = s1 * g1 + s3 * g3, s3 * g1 - s1 * g3
    out[1] = (r1 + u1, -(v1 + i1))
    out[7] = (r1 - u1, i1 - v1)
    out[3] = (r3 + u3, -(v3 + i3))
    out[5] = (r3 - u3, i3 - v3)
    return out


def transform_kernel(y_ref, table_ref, o_ref, lhs, mid):
    for g in range(ROWS // 16):
        rows = slice(16 * g, 16 * g + 16)
        dft = real_dft16([y_ref[a, rows, :] for a in range(PEERS)])
        for tile in range(8):
            pair = (dft[0][0], dft[8][0]) if tile == 0 else dft[tile]
            for part in range(2):
                high = pair[part].astype(jnp.bfloat16)
                low = (pair[part] - high.astype(jnp.float32)).astype(jnp.bfloat16)
                at = slice(128 * part, 128 * part + 128)
                lhs[tile, 16 * g : 16 * g + 16, at] = high
                lhs[tile, ROWS + 16 * g : ROWS + 16 * g + 16, at] = low
    dot = functools.partial(jnp.dot, preferred_element_type=jnp.float32)
    for tile in range(8):
        both = dot(lhs[tile], table_ref[0, tile])
        total = both[:ROWS] + both[ROWS:] + dot(lhs[tile, :ROWS, :], table_ref[1, tile])
        mid[tile] = total[:, :128]
        mid[8 if tile == 0 else PEERS - tile] = total[:, 128:]
    group = lax.broadcasted_iota(jnp.int32, (8, 128), 1) // 8
    bits = [(group >> s) % 2 == 1 for s in range(4)]
    for g in range(ROWS // 8):
        v = [mid[k, 8 * g : 8 * g + 8, :] for k in range(PEERS)]
        for s in range(4):
            v = [jnp.where(bits[s], v[(i + (1 << s)) % PEERS], v[i]) for i in range(PEERS)]
        latitude, radius = g // 2, 8 * (g % 2)
        for j in range(PEERS):
            value = v[-j % PEERS]
            if j:
                value = pltpu.roll(value, 128 - 8 * j, 1)
            at = NEAR * (j // 8) + Z * (j % 8) + FAR * (radius // 8) + latitude
            o_ref[pl.ds(at, 8, stride=REST), :] = value


def stage_kernel(table_ref, o_ref, sem):
    copy = pltpu.make_async_copy(table_ref, o_ref, sem)
    copy.start()
    copy.wait()


def stage(table):
    return pl.pallas_call(
        stage_kernel,
        out_shape=jax.ShapeDtypeStruct(table.shape, table.dtype),
        in_specs=[pl.BlockSpec(memory_space=pl.ANY)],
        out_specs=pl.BlockSpec(memory_space=pltpu.VMEM),
        scratch_shapes=[pltpu.SemaphoreType.DMA],
        compiler_params=pltpu.CompilerParams(vmem_limit_bytes=4 << 20),
        cost_estimate=pl.CostEstimate(flops=1 << 24, bytes_accessed=4 << 20, transcendentals=0),
        name="stage",
    )(table)


def transform(y, table):
    return pl.pallas_call(
        transform_kernel,
        out_shape=jax.ShapeDtypeStruct((1024, 128), jnp.float32),
        in_specs=[pl.BlockSpec(memory_space=pltpu.VMEM)] * 2,
        out_specs=pl.BlockSpec(memory_space=pltpu.VMEM),
        scratch_shapes=[
            pltpu.VMEM((8, 2 * ROWS, 256), jnp.bfloat16),
            pltpu.VMEM((PEERS, ROWS, 128), jnp.float32),
        ],
        compiler_params=pltpu.CompilerParams(vmem_limit_bytes=16 << 20),
        cost_estimate=pl.CostEstimate(flops=2 * 8 * 192 * 256 * 256, bytes_accessed=3 << 20, transcendentals=0),
        name="transform",
    )(y, table)


def weigh_kernel(g_ref, w_ref, re_ref, im_ref, turned, real, imag, sems):
    weights = w_ref[...]
    copies = []
    for f in range(4):
        for half in range(2):
            starts = [
                NEAR * ((4 * f + q) // 8) + Z * ((4 * f + q) % 8) + FAR * half + REST * i
                for i in range(8)
                for q in range(4)
            ]
            rows = jnp.concatenate([g_ref[start : start + 4, :] for start in starts], axis=0)
            at = slice(128 * half, 128 * half + 128)
            turned[f, half] = rows.T * weights[:, at]
            for step in range(4):
                real[f, 16 * step : 16 * step + 16, at] = turned[f, half, pl.ds(step, 16, stride=8), :]
                imag[f, 16 * step : 16 * step + 16, at] = turned[f, half, pl.ds(4 + step, 16, stride=8), :]
        copies.append(pltpu.make_async_copy(real.at[f], re_ref.at[f], sems.at[0, f]))
        copies.append(pltpu.make_async_copy(imag.at[f], im_ref.at[f], sems.at[1, f]))
        for copy in copies[-2:]:
            copy.start()
    for copy in copies:
        copy.wait()


def weigh(g, lat_weight):
    shape = jax.ShapeDtypeStruct((4, 64, 256), jnp.float32)
    return pl.pallas_call(
        weigh_kernel,
        out_shape=(shape, shape),
        in_specs=[pl.BlockSpec(memory_space=pltpu.VMEM)] * 2,
        out_specs=(pl.BlockSpec(memory_space=pltpu.HBM),) * 2,
        scratch_shapes=[
            pltpu.VMEM((4, 2, 128, 128), jnp.float32),
            pltpu.VMEM((4, 64, 256), jnp.float32),
            pltpu.VMEM((4, 64, 256), jnp.float32),
            pltpu.SemaphoreType.DMA((2, 4)),
        ],
        compiler_params=pltpu.CompilerParams(vmem_limit_bytes=16 << 20),
        cost_estimate=pl.CostEstimate(flops=1 << 18, bytes_accessed=1 << 20, transcendentals=0),
        name="weigh",
    )(g, lat_weight.reshape(1, 256))


def per_device(grid_field, lat_weight):
    y = lax.all_to_all(grid_field.reshape(16, 64, 128), ("near", "z"), 0, 0, tiled=True)
    z = transform(y, stage(jnp.asarray(mode_tables())))
    g = lax.all_to_all(z.reshape(256, 4, 128), ("z", "far", "near", "rest"), 0, 0, tiled=True)
    real, imag = weigh(g.reshape(1024, 128), lat_weight)
    return tuple(part.transpose(0, 2, 1)[:, :, None, :] for part in (real, imag))


def solution(mesh):
    mesh = jax.sharding.Mesh(mesh.devices.reshape(2, 8, 2, 8), ("near", "z", "far", "rest"))
    lon, lat = ("near", "z"), ("far", "rest")
    in_specs = (P(None, lat, None, lon), P())
    out_specs = (P(None, None, lat, lon), P(None, None, lat, lon))
    return jax.shard_map(per_device, mesh=mesh, in_specs=in_specs, out_specs=out_specs, check_vma=False)
```

```python
import functools
import math

import jax
import jax.numpy as jnp
import numpy as np
from jax import lax
from jax.experimental import pallas as pl
from jax.experimental.pallas import tpu as pltpu
from jax.sharding import PartitionSpec as P

LENGTH = 2048
PEERS = 16
BLOCK = 128
Z, FAR, NEAR, REST = 128, 64, 32, 4
ROWS = 64


ORDER = [8 * near + (z + 4) % 8 for near in range(2) for z in range(8)]


def mode_tables():
    b = np.arange(BLOCK)
    tables = np.zeros((8, 256, 256))
    for residue in range(PEERS):
        group, e = np.divmod(np.arange(128), 8)
        part, step = np.divmod(e, 4)
        owner = (group - residue) % PEERS
        mode = residue + PEERS * (4 * owner + step)
        phase = 2.0 * math.pi * (b[:, None] * mode[None, :] % LENGTH) / LENGTH
        cosine = np.cos(phase) / math.sqrt(LENGTH)
        sine = np.sin(phase) / math.sqrt(LENGTH)
        sign = -1.0 if residue > 8 else 1.0
        from_real = np.where(part == 0, cosine, -sine)
        from_imag = sign * np.where(part == 0, sine, cosine)
        if residue == 0:
            tables[0, :128, :128] = from_real
        elif residue == 8:
            tables[0, 128:, 128:] = from_real
        else:
            tile = min(residue, PEERS - residue)
            at = 0 if residue < 8 else 128
            tables[tile, :128, at : at + 128] = from_real
            tables[tile, 128:, at : at + 128] = from_imag
    table = tables.astype(np.float32)
    high = table.astype(jnp.bfloat16)
    low = (table - high.astype(np.float32)).astype(jnp.bfloat16)
    return np.stack([high, low])


def real_dft16(x):
    h = math.sqrt(0.5)
    c1, c3 = math.cos(math.pi / 8), math.cos(3 * math.pi / 8)
    s1, s3 = math.sin(math.pi / 8), math.sin(3 * math.pi / 8)
    s = [x[a] + x[a + 8] for a in range(8)]
    d = [x[a] - x[a + 8] for a in range(8)]
    p = [s[a] + s[a + 4] for a in range(4)]
    q = [s[a] - s[a + 4] for a in range(4)]
    out = [None] * 9
    even, odd = p[0] + p[2], p[1] + p[3]
    out[0] = (even + odd, None)
    out[8] = (even - odd, None)
    out[4] = (p[0] - p[2], p[3] - p[1])
    diff, total = h * (q[1] - q[3]), h * (q[1] + q[3])
    out[2] = (q[0] + diff, -q[2] - total)
    out[6] = (q[0] - diff, q[2] - total)
    e1, e2, e3 = d[1] - d[7], h * (d[2] - d[6]), d[3] - d[5]
    g1, g2, g3 = d[1] + d[7], h * (d[2] + d[6]), d[3] + d[5]
    r1, r3 = d[0] + e2, d[0] - e2
    u1, u3 = c1 * e1 + c3 * e3, c3 * e1 - c1 * e3
    i1, i3 = g2 + d[4], g2 - d[4]
    v1, v3 = s1 * g1 + s3 * g3, s3 * g1 - s1 * g3
    out[1] = (r1 + u1, -(v1 + i1))
    out[7] = (r1 - u1, i1 - v1)
    out[3] = (r3 + u3, -(v3 + i3))
    out[5] = (r3 - u3, i3 - v3)
    return out


def transform_kernel(y_ref, table_ref, o_ref, lhs, mid):
    for g in range(ROWS // 16):
        rows = slice(16 * g, 16 * g + 16)
        dft = real_dft16([y_ref[ORDER.index(a), rows, :] for a in range(PEERS)])
        for tile in range(8):
            pair = (dft[0][0], dft[8][0]) if tile == 0 else dft[tile]
            for part in range(2):
                high = pair[part].astype(jnp.bfloat16)
                low = (pair[part] - high.astype(jnp.float32)).astype(jnp.bfloat16)
                at = slice(128 * part, 128 * part + 128)
                lhs[tile, 16 * g : 16 * g + 16, at] = high
                lhs[tile, ROWS + 16 * g : ROWS + 16 * g + 16, at] = low
    dot = functools.partial(jnp.dot, preferred_element_type=jnp.float32)
    for tile in range(8):
        both = dot(lhs[tile], table_ref[0, tile])
        total = both[:ROWS] + both[ROWS:] + dot(lhs[tile, :ROWS, :], table_ref[1, tile])
        mid[tile] = total[:, :128]
        mid[8 if tile == 0 else PEERS - tile] = total[:, 128:]
    group = lax.broadcasted_iota(jnp.int32, (8, 128), 1) // 8
    bits = [(group >> s) % 2 == 1 for s in range(4)]
    for g in range(ROWS // 8):
        v = [mid[k, 8 * g : 8 * g + 8, :] for k in range(PEERS)]
        for s in range(4):
            v = [jnp.where(bits[s], v[(i + (1 << s)) % PEERS], v[i]) for i in range(PEERS)]
        latitude, radius = g // 2, 8 * (g % 2)
        for j in range(PEERS):
            value = v[-j % PEERS]
            if j:
                value = pltpu.roll(value, 128 - 8 * j, 1)
            at = NEAR * (j // 8) + Z * (j % 8) + FAR * (radius // 8) + latitude
            o_ref[pl.ds(at, 8, stride=REST), :] = value


def stage_kernel(table_ref, o_ref, sem):
    copy = pltpu.make_async_copy(table_ref, o_ref, sem)
    copy.start()
    copy.wait()


def stage(table):
    return pl.pallas_call(
        stage_kernel,
        out_shape=jax.ShapeDtypeStruct(table.shape, table.dtype),
        in_specs=[pl.BlockSpec(memory_space=pl.ANY)],
        out_specs=pl.BlockSpec(memory_space=pltpu.VMEM),
        scratch_shapes=[pltpu.SemaphoreType.DMA],
        compiler_params=pltpu.CompilerParams(vmem_limit_bytes=4 << 20),
        cost_estimate=pl.CostEstimate(flops=1 << 24, bytes_accessed=4 << 20, transcendentals=0),
        name="stage",
    )(table)


def transform(y, table):
    return pl.pallas_call(
        transform_kernel,
        out_shape=jax.ShapeDtypeStruct((1024, 128), jnp.float32),
        in_specs=[pl.BlockSpec(memory_space=pltpu.VMEM)] * 2,
        out_specs=pl.BlockSpec(memory_space=pltpu.VMEM),
        scratch_shapes=[
            pltpu.VMEM((8, 2 * ROWS, 256), jnp.bfloat16),
            pltpu.VMEM((PEERS, ROWS, 128), jnp.float32),
        ],
        compiler_params=pltpu.CompilerParams(vmem_limit_bytes=16 << 20),
        cost_estimate=pl.CostEstimate(flops=2 * 8 * 192 * 256 * 256, bytes_accessed=3 << 20, transcendentals=0),
        name="transform",
    )(y, table)


def weigh_kernel(g_ref, w_ref, re_ref, im_ref, turned, real, imag, sems):
    weights = w_ref[...]
    copies = []
    for f in range(4):
        for half in range(2):
            starts = [
                NEAR * (ORDER[4 * f + q] // 8) + Z * (ORDER[4 * f + q] % 8) + FAR * half + REST * i
                for i in range(8)
                for q in range(4)
            ]
            rows = jnp.concatenate([g_ref[start : start + 4, :] for start in starts], axis=0)
            at = slice(128 * half, 128 * half + 128)
            turned[f, half] = rows.T * weights[:, at]
            for step in range(4):
                real[f, 16 * step : 16 * step + 16, at] = turned[f, half, pl.ds(step, 16, stride=8), :]
                imag[f, 16 * step : 16 * step + 16, at] = turned[f, half, pl.ds(4 + step, 16, stride=8), :]
        copies.append(pltpu.make_async_copy(real.at[f], re_ref.at[f], sems.at[0, f]))
        copies.append(pltpu.make_async_copy(imag.at[f], im_ref.at[f], sems.at[1, f]))
        for copy in copies[-2:]:
            copy.start()
    for copy in copies:
        copy.wait()


def weigh(g, lat_weight):
    shape = jax.ShapeDtypeStruct((4, 64, 256), jnp.float32)
    return pl.pallas_call(
        weigh_kernel,
        out_shape=(shape, shape),
        in_specs=[pl.BlockSpec(memory_space=pltpu.VMEM)] * 2,
        out_specs=(pl.BlockSpec(memory_space=pltpu.HBM),) * 2,
        scratch_shapes=[
            pltpu.VMEM((4, 2, 128, 128), jnp.float32),
            pltpu.VMEM((4, 64, 256), jnp.float32),
            pltpu.VMEM((4, 64, 256), jnp.float32),
            pltpu.SemaphoreType.DMA((2, 4)),
        ],
        compiler_params=pltpu.CompilerParams(vmem_limit_bytes=16 << 20),
        cost_estimate=pl.CostEstimate(flops=1 << 18, bytes_accessed=1 << 20, transcendentals=0),
        name="weigh",
    )(g, lat_weight.reshape(1, 256))


def per_device(grid_field, lat_weight):
    y = lax.all_to_all(grid_field.reshape(16, 64, 128), ("near", "z"), 0, 0, tiled=True, axis_index_groups=[ORDER])
    z = transform(y, stage(jnp.asarray(mode_tables())))
    g = lax.all_to_all(z.reshape(256, 1, 512), ("z", "far", "near", "rest"), 0, 0, tiled=True)
    real, imag = weigh(g.reshape(1024, 128), lat_weight)
    return tuple(part.transpose(0, 2, 1)[:, :, None, :] for part in (real, imag))


def solution(mesh):
    mesh = jax.sharding.Mesh(mesh.devices.reshape(2, 8, 2, 8), ("near", "z", "far", "rest"))
    lon, lat = ("near", "z"), ("far", "rest")
    in_specs = (P(None, lat, None, lon), P())
    out_specs = (P(None, None, lat, lon), P(None, None, lat, lon))
    return jax.shard_map(per_device, mesh=mesh, in_specs=in_specs, out_specs=out_specs, check_vma=False)
```

```python
import functools
import math

import jax
import jax.numpy as jnp
import numpy as np
from jax import lax
from jax.experimental import pallas as pl
from jax.experimental.pallas import tpu as pltpu
from jax.sharding import PartitionSpec as P

LENGTH = 2048
PEERS = 16
BLOCK = 128
ROWS = 64


LON = [8 * near + (z + 4) % 8 for near in range(2) for z in range(8)]
FARS = [1, 0]


def place(rest, lon):
    near, z = divmod(lon, 8)
    return 8 * ((z - 4) % 8) + 64 * near + 1 * ((rest - 4) % 8)


def first():
    return [[16 * far + lon for far in FARS for lon in LON]]


def second():
    order = np.empty(128, np.int64)
    for device, parts in enumerate(np.ndindex(8, 16)):
        order[place(*parts)] = device
    return [[int(device) for device in order]]


def mode_tables():
    b = np.arange(BLOCK)
    tables = np.zeros((8, 256, 256))
    for residue in range(PEERS):
        group, e = np.divmod(np.arange(128), 8)
        part, step = np.divmod(e, 4)
        owner = (group - residue) % PEERS
        mode = residue + PEERS * (4 * owner + step)
        phase = 2.0 * math.pi * (b[:, None] * mode[None, :] % LENGTH) / LENGTH
        cosine = np.cos(phase) / math.sqrt(LENGTH)
        sine = np.sin(phase) / math.sqrt(LENGTH)
        sign = -1.0 if residue > 8 else 1.0
        from_real = np.where(part == 0, cosine, -sine)
        from_imag = sign * np.where(part == 0, sine, cosine)
        if residue == 0:
            tables[0, :128, :128] = from_real
        elif residue == 8:
            tables[0, 128:, 128:] = from_real
        else:
            tile = min(residue, PEERS - residue)
            at = 0 if residue < 8 else 128
            tables[tile, :128, at : at + 128] = from_real
            tables[tile, 128:, at : at + 128] = from_imag
    table = tables.astype(np.float32)
    high = table.astype(jnp.bfloat16)
    low = (table - high.astype(np.float32)).astype(jnp.bfloat16)
    return np.stack([high, low])


def real_dft16(x):
    h = math.sqrt(0.5)
    c1, c3 = math.cos(math.pi / 8), math.cos(3 * math.pi / 8)
    s1, s3 = math.sin(math.pi / 8), math.sin(3 * math.pi / 8)
    s = [x[a] + x[a + 8] for a in range(8)]
    d = [x[a] - x[a + 8] for a in range(8)]
    p = [s[a] + s[a + 4] for a in range(4)]
    q = [s[a] - s[a + 4] for a in range(4)]
    out = [None] * 9
    even, odd = p[0] + p[2], p[1] + p[3]
    out[0] = (even + odd, None)
    out[8] = (even - odd, None)
    out[4] = (p[0] - p[2], p[3] - p[1])
    diff, total = h * (q[1] - q[3]), h * (q[1] + q[3])
    out[2] = (q[0] + diff, -q[2] - total)
    out[6] = (q[0] - diff, q[2] - total)
    e1, e2, e3 = d[1] - d[7], h * (d[2] - d[6]), d[3] - d[5]
    g1, g2, g3 = d[1] + d[7], h * (d[2] + d[6]), d[3] + d[5]
    r1, r3 = d[0] + e2, d[0] - e2
    u1, u3 = c1 * e1 + c3 * e3, c3 * e1 - c1 * e3
    i1, i3 = g2 + d[4], g2 - d[4]
    v1, v3 = s1 * g1 + s3 * g3, s3 * g1 - s1 * g3
    out[1] = (r1 + u1, -(v1 + i1))
    out[7] = (r1 - u1, i1 - v1)
    out[3] = (r3 + u3, -(v3 + i3))
    out[5] = (r3 - u3, i3 - v3)
    return out


def transform_kernel(y_ref, table_ref, o_ref, lhs, mid):
    for g in range(ROWS // 16):
        far, inner = divmod(16 * g, 32)
        dft = real_dft16([y_ref[FARS.index(far) * PEERS + LON.index(a), inner : inner + 16, :] for a in range(PEERS)])
        for tile in range(8):
            pair = (dft[0][0], dft[8][0]) if tile == 0 else dft[tile]
            for part in range(2):
                high = pair[part].astype(jnp.bfloat16)
                low = (pair[part] - high.astype(jnp.float32)).astype(jnp.bfloat16)
                at = slice(128 * part, 128 * part + 128)
                lhs[tile, 16 * g : 16 * g + 16, at] = high
                lhs[tile, ROWS + 16 * g : ROWS + 16 * g + 16, at] = low
    dot = functools.partial(jnp.dot, preferred_element_type=jnp.float32)
    for tile in range(8):
        both = dot(lhs[tile], table_ref[0, tile])
        total = both[:ROWS] + both[ROWS:] + dot(lhs[tile, :ROWS, :], table_ref[1, tile])
        mid[tile] = total[:, :128]
        mid[8 if tile == 0 else PEERS - tile] = total[:, 128:]
    group = lax.broadcasted_iota(jnp.int32, (8, 128), 1) // 8
    bits = [(group >> s) % 2 == 1 for s in range(4)]
    for g in range(ROWS // 8):
        v = [mid[k, 8 * g : 8 * g + 8, :] for k in range(PEERS)]
        for s in range(4):
            v = [jnp.where(bits[s], v[(i + (1 << s)) % PEERS], v[i]) for i in range(PEERS)]
        for j in range(PEERS):
            value = v[-j % PEERS]
            if j:
                value = pltpu.roll(value, 128 - 8 * j, 1)
            for rest in (0, 4):
                o_ref[pl.ds(8 * place(rest, j) + g, 4, stride=8), :] = value[rest : rest + 4]


def stage_kernel(table_ref, o_ref, sem):
    copy = pltpu.make_async_copy(table_ref, o_ref, sem)
    copy.start()
    copy.wait()


def stage(table):
    return pl.pallas_call(
        stage_kernel,
        out_shape=jax.ShapeDtypeStruct(table.shape, table.dtype),
        in_specs=[pl.BlockSpec(memory_space=pl.ANY)],
        out_specs=pl.BlockSpec(memory_space=pltpu.VMEM),
        scratch_shapes=[pltpu.SemaphoreType.DMA],
        compiler_params=pltpu.CompilerParams(vmem_limit_bytes=4 << 20),
        cost_estimate=pl.CostEstimate(flops=1 << 24, bytes_accessed=4 << 20, transcendentals=0),
        name="stage",
    )(table)


def transform(y, table):
    return pl.pallas_call(
        transform_kernel,
        out_shape=jax.ShapeDtypeStruct((1024, 128), jnp.float32),
        in_specs=[pl.BlockSpec(memory_space=pltpu.VMEM)] * 2,
        out_specs=pl.BlockSpec(memory_space=pltpu.VMEM),
        scratch_shapes=[
            pltpu.VMEM((8, 2 * ROWS, 256), jnp.bfloat16),
            pltpu.VMEM((PEERS, ROWS, 128), jnp.float32),
        ],
        compiler_params=pltpu.CompilerParams(vmem_limit_bytes=16 << 20),
        cost_estimate=pl.CostEstimate(flops=2 * 8 * 192 * 256 * 256, bytes_accessed=3 << 20, transcendentals=0),
        name="transform",
    )(y, table)


def weigh_kernel(g_ref, w_ref, re_ref, im_ref, turned, real, imag, sems):
    weights = w_ref[...]
    copies = []
    for f in range(4):
        for half in range(2):
            starts = [8 * place(i, LON[4 * f + q]) + 4 * half for i in range(8) for q in range(4)]
            rows = jnp.concatenate([g_ref[start : start + 4, :] for start in starts], axis=0)
            at = slice(128 * half, 128 * half + 128)
            turned[f, half] = rows.T * weights[:, at]
            for step in range(4):
                real[f, 16 * step : 16 * step + 16, at] = turned[f, half, pl.ds(step, 16, stride=8), :]
                imag[f, 16 * step : 16 * step + 16, at] = turned[f, half, pl.ds(4 + step, 16, stride=8), :]
        copies.append(pltpu.make_async_copy(real.at[f], re_ref.at[f], sems.at[0, f]))
        copies.append(pltpu.make_async_copy(imag.at[f], im_ref.at[f], sems.at[1, f]))
        for copy in copies[-2:]:
            copy.start()
    for copy in copies:
        copy.wait()


def weigh(g, lat_weight):
    shape = jax.ShapeDtypeStruct((4, 64, 256), jnp.float32)
    return pl.pallas_call(
        weigh_kernel,
        out_shape=(shape, shape),
        in_specs=[pl.BlockSpec(memory_space=pltpu.VMEM)] * 2,
        out_specs=(pl.BlockSpec(memory_space=pltpu.HBM),) * 2,
        scratch_shapes=[
            pltpu.VMEM((4, 2, 128, 128), jnp.float32),
            pltpu.VMEM((4, 64, 256), jnp.float32),
            pltpu.VMEM((4, 64, 256), jnp.float32),
            pltpu.SemaphoreType.DMA((2, 4)),
        ],
        compiler_params=pltpu.CompilerParams(vmem_limit_bytes=16 << 20),
        cost_estimate=pl.CostEstimate(flops=1 << 18, bytes_accessed=1 << 20, transcendentals=0),
        name="weigh",
    )(g, lat_weight.reshape(1, 256))


def per_device(grid_field, lat_weight):
    table = stage(jnp.asarray(mode_tables()))
    y = lax.all_to_all(grid_field.reshape(64, 2, 8, 128)[:, ::-1].transpose(1, 0, 2, 3).reshape(32, 32, 128), ("far", "lon"), 0, 0, tiled=True, axis_index_groups=first())
    z = transform(y, table)
    g = lax.all_to_all(z.reshape(128, 8, 128), ("near", "lon"), 0, 0, tiled=True, axis_index_groups=second())
    real, imag = weigh(g.reshape(1024, 128), lat_weight)
    return tuple(part.transpose(0, 2, 1)[:, :, None, :] for part in (real, imag))


def solution(mesh):
    mesh = jax.sharding.Mesh(mesh.devices.reshape(16, 2, 8), ("lon", "far", "near"))
    lat = ("far", "near")
    in_specs = (P(None, lat, None, "lon"), P())
    out_specs = (P(None, None, lat, "lon"), P(None, None, lat, "lon"))
    return jax.shard_map(per_device, mesh=mesh, in_specs=in_specs, out_specs=out_specs, check_vma=False)
```

```python
import functools
import math

import jax
import jax.numpy as jnp
import numpy as np
from jax import lax
from jax.experimental import pallas as pl
from jax.experimental.pallas import tpu as pltpu
from jax.sharding import PartitionSpec as P

LENGTH = 2048
PEERS = 16
BLOCK = 128
ROWS = 64

LON = [8 * near + (z + 4) % 8 for near in range(2) for z in range(8)]
FARS = [1, 0]


def place(rest, lon):
    near, z = divmod(lon, 8)
    return 16 * ((z - 4) % 8) + 8 * (1 - near) + (rest - 5) % 8


def first():
    return [[16 * far + lon for far in FARS for lon in LON]]


def second():
    order = np.empty(128, np.int64)
    for device, parts in enumerate(np.ndindex(8, 16)):
        order[place(*parts)] = device
    return [[int(device) for device in order]]


def mode_tables():
    b = np.arange(BLOCK)
    tables = np.zeros((8, 256, 256))
    for residue in range(PEERS):
        group, e = np.divmod(np.arange(128), 8)
        part, step = np.divmod(e, 4)
        owner = (group - residue) % PEERS
        mode = residue + PEERS * (4 * owner + step)
        phase = 2.0 * math.pi * (b[:, None] * mode[None, :] % LENGTH) / LENGTH
        cosine = np.cos(phase) / math.sqrt(LENGTH)
        sine = np.sin(phase) / math.sqrt(LENGTH)
        sign = -1.0 if residue > 8 else 1.0
        from_real = np.where(part == 0, cosine, -sine)
        from_imag = sign * np.where(part == 0, sine, cosine)
        if residue == 0:
            tables[0, :128, :128] = from_real
        elif residue == 8:
            tables[0, 128:, 128:] = from_real
        else:
            tile = min(residue, PEERS - residue)
            at = 0 if residue < 8 else 128
            tables[tile, :128, at : at + 128] = from_real
            tables[tile, 128:, at : at + 128] = from_imag
    table = tables.astype(np.float32)
    high = table.astype(jnp.bfloat16)
    low = (table - high.astype(np.float32)).astype(jnp.bfloat16)
    return np.stack([high, low])


def real_dft16(x):
    h = math.sqrt(0.5)
    c1, c3 = math.cos(math.pi / 8), math.cos(3 * math.pi / 8)
    s1, s3 = math.sin(math.pi / 8), math.sin(3 * math.pi / 8)
    s = [x[a] + x[a + 8] for a in range(8)]
    d = [x[a] - x[a + 8] for a in range(8)]
    p = [s[a] + s[a + 4] for a in range(4)]
    q = [s[a] - s[a + 4] for a in range(4)]
    out = [None] * 9
    even, odd = p[0] + p[2], p[1] + p[3]
    out[0] = (even + odd, None)
    out[8] = (even - odd, None)
    out[4] = (p[0] - p[2], p[3] - p[1])
    diff, total = h * (q[1] - q[3]), h * (q[1] + q[3])
    out[2] = (q[0] + diff, -q[2] - total)
    out[6] = (q[0] - diff, q[2] - total)
    e1, e2, e3 = d[1] - d[7], h * (d[2] - d[6]), d[3] - d[5]
    g1, g2, g3 = d[1] + d[7], h * (d[2] + d[6]), d[3] + d[5]
    r1, r3 = d[0] + e2, d[0] - e2
    u1, u3 = c1 * e1 + c3 * e3, c3 * e1 - c1 * e3
    i1, i3 = g2 + d[4], g2 - d[4]
    v1, v3 = s1 * g1 + s3 * g3, s3 * g1 - s1 * g3
    out[1] = (r1 + u1, -(v1 + i1))
    out[7] = (r1 - u1, i1 - v1)
    out[3] = (r3 + u3, -(v3 + i3))
    out[5] = (r3 - u3, i3 - v3)
    return out


def transform_kernel(y_ref, table_ref, o_ref, lhs, mid):
    for g in range(ROWS // 16):
        far, inner = divmod(16 * g, 32)
        dft = real_dft16([y_ref[FARS.index(far) * PEERS + LON.index(a), inner : inner + 16, :] for a in range(PEERS)])
        for tile in range(8):
            pair = (dft[0][0], dft[8][0]) if tile == 0 else dft[tile]
            for part in range(2):
                high = pair[part].astype(jnp.bfloat16)
                low = (pair[part] - high.astype(jnp.float32)).astype(jnp.bfloat16)
                at = slice(128 * part, 128 * part + 128)
                lhs[tile, 16 * g : 16 * g + 16, at] = high
                lhs[tile, ROWS + 16 * g : ROWS + 16 * g + 16, at] = low
    dot = functools.partial(jnp.dot, preferred_element_type=jnp.float32)
    for tile in range(8):
        both = dot(lhs[tile], table_ref[0, tile])
        total = both[:ROWS] + both[ROWS:] + dot(lhs[tile, :ROWS, :], table_ref[1, tile])
        mid[tile] = total[:, :128]
        mid[8 if tile == 0 else PEERS - tile] = total[:, 128:]
    group = lax.broadcasted_iota(jnp.int32, (8, 128), 1) // 8
    bits = [(group >> s) % 2 == 1 for s in range(4)]
    for g in range(ROWS // 8):
        v = [mid[k, 8 * g : 8 * g + 8, :] for k in range(PEERS)]
        for s in range(4):
            v = [jnp.where(bits[s], v[(i + (1 << s)) % PEERS], v[i]) for i in range(PEERS)]
        for j in range(PEERS):
            value = v[-j % PEERS]
            if j:
                value = pltpu.roll(value, 128 - 8 * j, 1)
            for rest, end in ((0, 5), (5, 8)):
                o_ref[pl.ds(8 * place(rest, j) + g, end - rest, stride=8), :] = value[rest:end]


def stage_kernel(table_ref, o_ref, sem):
    copy = pltpu.make_async_copy(table_ref, o_ref, sem)
    copy.start()
    copy.wait()


def stage(table):
    return pl.pallas_call(
        stage_kernel,
        out_shape=jax.ShapeDtypeStruct(table.shape, table.dtype),
        in_specs=[pl.BlockSpec(memory_space=pl.ANY)],
        out_specs=pl.BlockSpec(memory_space=pltpu.VMEM),
        scratch_shapes=[pltpu.SemaphoreType.DMA],
        compiler_params=pltpu.CompilerParams(vmem_limit_bytes=4 << 20),
        cost_estimate=pl.CostEstimate(flops=1 << 24, bytes_accessed=4 << 20, transcendentals=0),
        name="stage",
    )(table)


def transform(y, table):
    return pl.pallas_call(
        transform_kernel,
        out_shape=jax.ShapeDtypeStruct((1024, 128), jnp.float32),
        in_specs=[pl.BlockSpec(memory_space=pltpu.VMEM)] * 2,
        out_specs=pl.BlockSpec(memory_space=pltpu.VMEM),
        scratch_shapes=[
            pltpu.VMEM((8, 2 * ROWS, 256), jnp.bfloat16),
            pltpu.VMEM((PEERS, ROWS, 128), jnp.float32),
        ],
        compiler_params=pltpu.CompilerParams(vmem_limit_bytes=16 << 20),
        cost_estimate=pl.CostEstimate(flops=2 * 8 * 192 * 256 * 256, bytes_accessed=3 << 20, transcendentals=0),
        name="transform",
    )(y, table)


def weigh_kernel(g_ref, w_ref, re_ref, im_ref, turned, real, imag, sems):
    weights = w_ref[...]
    copies = []
    for f in range(4):
        for half in range(2):
            starts = [8 * place(i, LON[4 * f + q]) + 4 * half for i in range(8) for q in range(4)]
            rows = jnp.concatenate([g_ref[start : start + 4, :] for start in starts], axis=0)
            at = slice(128 * half, 128 * half + 128)
            turned[f, half] = rows.T * weights[:, at]
            for step in range(4):
                real[f, 16 * step : 16 * step + 16, at] = turned[f, half, pl.ds(step, 16, stride=8), :]
                imag[f, 16 * step : 16 * step + 16, at] = turned[f, half, pl.ds(4 + step, 16, stride=8), :]
        copies.append(pltpu.make_async_copy(real.at[f], re_ref.at[f], sems.at[0, f]))
        copies.append(pltpu.make_async_copy(imag.at[f], im_ref.at[f], sems.at[1, f]))
        for copy in copies[-2:]:
            copy.start()
    for copy in copies:
        copy.wait()


def weigh(g, lat_weight):
    shape = jax.ShapeDtypeStruct((4, 64, 256), jnp.float32)
    return pl.pallas_call(
        weigh_kernel,
        out_shape=(shape, shape),
        in_specs=[pl.BlockSpec(memory_space=pltpu.VMEM)] * 2,
        out_specs=(pl.BlockSpec(memory_space=pltpu.HBM),) * 2,
        scratch_shapes=[
            pltpu.VMEM((4, 2, 128, 128), jnp.float32),
            pltpu.VMEM((4, 64, 256), jnp.float32),
            pltpu.VMEM((4, 64, 256), jnp.float32),
            pltpu.SemaphoreType.DMA((2, 4)),
        ],
        compiler_params=pltpu.CompilerParams(vmem_limit_bytes=16 << 20),
        cost_estimate=pl.CostEstimate(flops=1 << 18, bytes_accessed=1 << 20, transcendentals=0),
        name="weigh",
    )(g, lat_weight.reshape(1, 256))


def per_device(grid_field, lat_weight):
    table = stage(jnp.asarray(mode_tables()))
    x = grid_field.reshape(64, 2, 8, 128)[:, ::-1].transpose(1, 0, 2, 3).reshape(32, 32, 128)
    y = lax.all_to_all(x, ("far", "lon"), 0, 0, tiled=True, axis_index_groups=first())
    z = transform(y, table)
    g = lax.all_to_all(z.reshape(128, 8, 128), ("near", "lon"), 0, 0, tiled=True, axis_index_groups=second())
    real, imag = weigh(g.reshape(1024, 128), lat_weight)
    return tuple(part.transpose(0, 2, 1)[:, :, None, :] for part in (real, imag))


def solution(mesh):
    mesh = jax.sharding.Mesh(mesh.devices.reshape(16, 2, 8), ("lon", "far", "near"))
    lat = ("far", "near")
    in_specs = (P(None, lat, None, "lon"), P())
    out_specs = (P(None, None, lat, "lon"), P(None, None, lat, "lon"))
    return jax.shard_map(per_device, mesh=mesh, in_specs=in_specs, out_specs=out_specs, check_vma=False)
```

```python
import functools
import math

import jax
import jax.numpy as jnp
import numpy as np
from jax import lax
from jax.experimental import pallas as pl
from jax.experimental.pallas import tpu as pltpu
from jax.sharding import PartitionSpec as P

LENGTH = 2048
PEERS = 16
BLOCK = 128
ROWS = 64

LON = [8 * near + (z + 4) % 8 for near in range(2) for z in range(8)]
FARS = [1, 0]


def place(rest, lon):
    near, z = divmod(lon, 8)
    return 16 * ((z - 4) % 8) + 8 * (1 - near) + (rest - 5) % 8


def first():
    return [[16 * far + lon for far in FARS for lon in LON]]


def second():
    order = np.empty(128, np.int64)
    for device, parts in enumerate(np.ndindex(8, 16)):
        order[place(*parts)] = device
    return [[int(device) for device in order]]


def mode_tables():
    b = np.arange(BLOCK)
    tables = np.zeros((8, 256, 256))
    for residue in range(PEERS):
        group, e = np.divmod(np.arange(128), 8)
        part, step = np.divmod(e, 4)
        owner = (group - residue) % PEERS
        mode = residue + PEERS * (4 * owner + step)
        phase = 2.0 * math.pi * (b[:, None] * mode[None, :] % LENGTH) / LENGTH
        cosine = np.cos(phase) / math.sqrt(LENGTH)
        sine = np.sin(phase) / math.sqrt(LENGTH)
        sign = -1.0 if residue > 8 else 1.0
        from_real = np.where(part == 0, cosine, -sine)
        from_imag = sign * np.where(part == 0, sine, cosine)
        if residue == 0:
            tables[0, :128, :128] = from_real
        elif residue == 8:
            tables[0, 128:, 128:] = from_real
        else:
            tile = min(residue, PEERS - residue)
            at = 0 if residue < 8 else 128
            tables[tile, :128, at : at + 128] = from_real
            tables[tile, 128:, at : at + 128] = from_imag
    table = tables.astype(np.float32)
    high = table.astype(jnp.bfloat16)
    low = (table - high.astype(np.float32)).astype(jnp.bfloat16)
    return np.stack([high, low])


def real_dft16(x):
    h = math.sqrt(0.5)
    c1, c3 = math.cos(math.pi / 8), math.cos(3 * math.pi / 8)
    s1, s3 = math.sin(math.pi / 8), math.sin(3 * math.pi / 8)
    s = [x[a] + x[a + 8] for a in range(8)]
    d = [x[a] - x[a + 8] for a in range(8)]
    p = [s[a] + s[a + 4] for a in range(4)]
    q = [s[a] - s[a + 4] for a in range(4)]
    out = [None] * 9
    even, odd = p[0] + p[2], p[1] + p[3]
    out[0] = (even + odd, None)
    out[8] = (even - odd, None)
    out[4] = (p[0] - p[2], p[3] - p[1])
    diff, total = h * (q[1] - q[3]), h * (q[1] + q[3])
    out[2] = (q[0] + diff, -q[2] - total)
    out[6] = (q[0] - diff, q[2] - total)
    e1, e2, e3 = d[1] - d[7], h * (d[2] - d[6]), d[3] - d[5]
    g1, g2, g3 = d[1] + d[7], h * (d[2] + d[6]), d[3] + d[5]
    r1, r3 = d[0] + e2, d[0] - e2
    u1, u3 = c1 * e1 + c3 * e3, c3 * e1 - c1 * e3
    i1, i3 = g2 + d[4], g2 - d[4]
    v1, v3 = s1 * g1 + s3 * g3, s3 * g1 - s1 * g3
    out[1] = (r1 + u1, -(v1 + i1))
    out[7] = (r1 - u1, i1 - v1)
    out[3] = (r3 + u3, -(v3 + i3))
    out[5] = (r3 - u3, i3 - v3)
    return out


def transform_kernel(y_ref, table_ref, o_ref, lhs, mid):
    for g in range(ROWS // 16):
        far, inner = divmod(16 * g, 32)
        dft = real_dft16([y_ref[FARS.index(far) * PEERS + LON.index(a), inner : inner + 16, :] for a in range(PEERS)])
        for tile in range(8):
            pair = (dft[0][0], dft[8][0]) if tile == 0 else dft[tile]
            for part in range(2):
                high = pair[part].astype(jnp.bfloat16)
                low = (pair[part] - high.astype(jnp.float32)).astype(jnp.bfloat16)
                at = slice(128 * part, 128 * part + 128)
                lhs[tile, 16 * g : 16 * g + 16, at] = high
                lhs[tile, ROWS + 16 * g : ROWS + 16 * g + 16, at] = low
    dot = functools.partial(jnp.dot, preferred_element_type=jnp.float32)
    for tile in range(8):
        both = dot(lhs[tile], table_ref[0, tile])
        total = both[:ROWS] + both[ROWS:] + dot(lhs[tile, :ROWS, :], table_ref[1, tile])
        mid[tile] = total[:, :128]
        mid[8 if tile == 0 else PEERS - tile] = total[:, 128:]
    group = lax.broadcasted_iota(jnp.int32, (8, 128), 1) // 8
    bits = [(group >> s) % 2 == 1 for s in range(4)]
    for g in range(ROWS // 8):
        v = [mid[k, 8 * g : 8 * g + 8, :] for k in range(PEERS)]
        for s in range(4):
            v = [jnp.where(bits[s], v[(i + (1 << s)) % PEERS], v[i]) for i in range(PEERS)]
        for j in range(PEERS):
            value = v[-j % PEERS]
            if j:
                value = pltpu.roll(value, 128 - 8 * j, 1)
            for rest, end in ((0, 5), (5, 8)):
                o_ref[pl.ds(8 * place(rest, j) + g, end - rest, stride=8), :] = value[rest:end]


def stage_kernel(table_ref, o_ref, sem):
    copy = pltpu.make_async_copy(table_ref, o_ref, sem)
    copy.start()
    copy.wait()


def stage(table):
    return pl.pallas_call(
        stage_kernel,
        out_shape=jax.ShapeDtypeStruct(table.shape, table.dtype),
        in_specs=[pl.BlockSpec(memory_space=pl.ANY)],
        out_specs=pl.BlockSpec(memory_space=pltpu.VMEM),
        scratch_shapes=[pltpu.SemaphoreType.DMA],
        compiler_params=pltpu.CompilerParams(vmem_limit_bytes=4 << 20),
        cost_estimate=pl.CostEstimate(flops=1 << 24, bytes_accessed=4 << 20, transcendentals=0),
        name="stage",
    )(table)


def transform(y, table):
    return pl.pallas_call(
        transform_kernel,
        out_shape=jax.ShapeDtypeStruct((1024, 128), jnp.float32),
        in_specs=[pl.BlockSpec(memory_space=pltpu.VMEM)] * 2,
        out_specs=pl.BlockSpec(memory_space=pltpu.VMEM),
        scratch_shapes=[
            pltpu.VMEM((8, 2 * ROWS, 256), jnp.bfloat16),
            pltpu.VMEM((PEERS, ROWS, 128), jnp.float32),
        ],
        compiler_params=pltpu.CompilerParams(vmem_limit_bytes=16 << 20),
        cost_estimate=pl.CostEstimate(flops=2 * 8 * 192 * 256 * 256, bytes_accessed=3 << 20, transcendentals=0),
        name="transform",
    )(y, table)


def pack_kernel(x_ref, o_ref, held, sems):
    pieces = [(i, slice(16 * part, 16 * part + 16)) for part in range(4) for i in range(2)]
    ins = [
        pltpu.make_async_copy(x_ref.at[rows, FARS[i]], held.at[i, rows], sems.at[0, n])
        for n, (i, rows) in enumerate(pieces)
    ]
    outs = [
        pltpu.make_async_copy(held.at[i, rows], o_ref.at[i, rows], sems.at[1, n]) for n, (i, rows) in enumerate(pieces)
    ]
    for copy in ins:
        copy.start()
    for into, out in zip(ins, outs):
        into.wait()
        out.start()
    for copy in outs:
        copy.wait()


def pack(x):
    return pl.pallas_call(
        pack_kernel,
        out_shape=jax.ShapeDtypeStruct((2, 64, 8, 128), jnp.float32),
        in_specs=[pl.BlockSpec(memory_space=pltpu.HBM)],
        out_specs=pl.BlockSpec(memory_space=pltpu.HBM),
        scratch_shapes=[pltpu.VMEM((2, 64, 8, 128), jnp.float32), pltpu.SemaphoreType.DMA((2, 8))],
        compiler_params=pltpu.CompilerParams(vmem_limit_bytes=66_300_000),
        cost_estimate=pl.CostEstimate(flops=1 << 18, bytes_accessed=1 << 20, transcendentals=0),
        name="pack",
    )(x.reshape(64, 2, 8, 128))


def weigh_kernel(g_ref, w_ref, re_ref, im_ref, turned, real, imag, sems):
    weights = w_ref[...]
    copies = []
    for f in range(4):
        for half in range(2):
            starts = [8 * place(i, LON[4 * f + q]) + 4 * half for i in range(8) for q in range(4)]
            rows = jnp.concatenate([g_ref[start : start + 4, :] for start in starts], axis=0)
            at = slice(128 * half, 128 * half + 128)
            turned[f, half] = rows.T * weights[:, at]
            for step in range(4):
                real[f, 16 * step : 16 * step + 16, at] = turned[f, half, pl.ds(step, 16, stride=8), :]
                imag[f, 16 * step : 16 * step + 16, at] = turned[f, half, pl.ds(4 + step, 16, stride=8), :]
        copies.append(pltpu.make_async_copy(real.at[f], re_ref.at[f], sems.at[0, f]))
        copies.append(pltpu.make_async_copy(imag.at[f], im_ref.at[f], sems.at[1, f]))
        for copy in copies[-2:]:
            copy.start()
    for copy in copies:
        copy.wait()


def weigh(g, lat_weight):
    shape = jax.ShapeDtypeStruct((4, 64, 256), jnp.float32)
    return pl.pallas_call(
        weigh_kernel,
        out_shape=(shape, shape),
        in_specs=[pl.BlockSpec(memory_space=pltpu.VMEM)] * 2,
        out_specs=(pl.BlockSpec(memory_space=pltpu.HBM),) * 2,
        scratch_shapes=[
            pltpu.VMEM((4, 2, 128, 128), jnp.float32),
            pltpu.VMEM((4, 64, 256), jnp.float32),
            pltpu.VMEM((4, 64, 256), jnp.float32),
            pltpu.SemaphoreType.DMA((2, 4)),
        ],
        compiler_params=pltpu.CompilerParams(vmem_limit_bytes=16 << 20),
        cost_estimate=pl.CostEstimate(flops=1 << 18, bytes_accessed=1 << 20, transcendentals=0),
        name="weigh",
    )(g, lat_weight.reshape(1, 256))


def per_device(grid_field, lat_weight):
    table = stage(jnp.asarray(mode_tables()))
    x = pack(grid_field).reshape(32, 32, 128)
    y = lax.all_to_all(x, ("far", "lon"), 0, 0, tiled=True, axis_index_groups=first())
    z = transform(y, table)
    g = lax.all_to_all(z.reshape(128, 8, 128), ("near", "lon"), 0, 0, tiled=True, axis_index_groups=second())
    real, imag = weigh(g.reshape(1024, 128), lat_weight)
    return tuple(part.transpose(0, 2, 1)[:, :, None, :] for part in (real, imag))


def solution(mesh):
    mesh = jax.sharding.Mesh(mesh.devices.reshape(16, 2, 8), ("lon", "far", "near"))
    lat = ("far", "near")
    in_specs = (P(None, lat, None, "lon"), P())
    out_specs = (P(None, None, lat, "lon"), P(None, None, lat, "lon"))
    return jax.shard_map(per_device, mesh=mesh, in_specs=in_specs, out_specs=out_specs, check_vma=False)
```
